32 devices in a mesh: fsdp: 2 (over y), trow: 4 (over x, core), tcol: 4 (over z).
Axes of the slice: x: 2, y: 2, z: 4, core: 2. Of those that a mesh axis runs over, the one named last changes fastest.
Arguments:
- tokens: bfloat16 [512, 4096], P('fsdp', 'tcol'), may hold values from -100 to 100
- w_up: bfloat16 [4096, 16384], P('tcol', ('fsdp', 'trow')), may hold values from -0.1875 to 0.1875
- w_down: bfloat16 [16384, 4096], P(('fsdp', 'trow'), 'tcol'), may hold values from -0.046875 to 0.046875
- cotangent: bfloat16 [512, 4096], P('fsdp', 'tcol'), may hold values from -6 to 6
Outputs:
- mixed: bfloat16 [512, 4096], P('fsdp', 'tcol')
- input_gradient: bfloat16 [512, 4096], P('fsdp', 'tcol')
- grad_up: bfloat16 [4096, 16384], P('tcol', ('fsdp', 'trow'))
- grad_down: bfloat16 [16384, 4096], P(('fsdp', 'trow'), 'tcol')
The draws below stay inside these ranges and needn't reach their ends.
All inputs are finite; a program needn't handle non-finite values.
Results may differ from the reference program's by a relative error of at most 0.02.
Values may be sent and summed in bfloat16 or wider, within the bound.
A program may use at most 128 MiB of HBM per device.

```python
import jax
import jax.numpy as jnp
from jax import lax

MODEL_WIDTH = 4096
FF = 16384
TOK_GRP = 256
TOKENS = 512
N_FSDP = 2
N_TCOL = 4


def draw_tokens(key, part):
    keys = jax.random.split(jax.random.fold_in(key, 17), 3)
    rising = jnp.exp(jnp.log(3.0) * jnp.arange(MODEL_WIDTH, dtype=jnp.float32) / (MODEL_WIDTH - 1))
    column = rising * jnp.exp(jax.random.uniform(keys[1], (MODEL_WIDTH,), jnp.float32, 0.0, jnp.log(10.0))) / jnp.sqrt(30.0)
    base = jnp.clip(jax.random.normal(keys[0], (TOKENS, MODEL_WIDTH), jnp.float32), -4.0, 4.0)
    row = jnp.exp(jax.random.uniform(keys[2], (TOKENS, 1), jnp.float32, 0.0, jnp.log(10.0))) / jnp.sqrt(10.0)
    return (base * row * column[None, :]).astype(jnp.bfloat16)


def draw_w_up(key, part):
    keys = jax.random.split(jax.random.fold_in(key, 29), 2)
    position = jnp.arange(MODEL_WIDTH, dtype=jnp.float32) / (MODEL_WIDTH - 1)
    shared = jnp.clip(jax.random.normal(keys[1], (1, FF), jnp.float32), -3.0, 3.0)
    rising = jnp.exp(jnp.log(4.0) * position)
    noise = jnp.clip(jax.random.normal(keys[0], (MODEL_WIDTH, FF), jnp.float32), -4.0, 4.0)
    strength = 0.5
    rising = rising / jnp.sqrt(jnp.mean(rising * rising))
    values = rising[:, None] * (noise + strength * shared) / jnp.sqrt(1.0 * MODEL_WIDTH)
    return values.astype(jnp.bfloat16)


def shard_levels(own_key, dims, cuts, low, high):
    def one(dim, parts):
        steps = jax.random.uniform(jax.random.fold_in(jax.random.fold_in(own_key, 6), dim), (parts,), jnp.float32, low / len(cuts), high / len(cuts))
        return jnp.repeat(jnp.exp(steps), dims[dim] // parts).reshape((-1,) + (1,) * (len(dims) - dim - 1))

    level = one(*cuts[0])
    for cut in cuts[1:]:
        level = level * one(*cut)
    return level


def bell_draw(stream_key, shape, spread, reach, shards=(), kind=jnp.bfloat16):
    result = spread * jax.random.normal(stream_key, shape, jnp.float32)
    if shards:
        result = result * shard_levels(stream_key, shape, shards, -0.22, 0.18)
    return jnp.clip(result, -reach, reach).astype(kind)


def setup_inputs(seed: int = 0) -> dict:
    key_of = jax.random.split(jax.random.key(seed), 5)
    return {
        "tokens": draw_tokens(jax.random.fold_in(key_of[4], 71), 0),
        "w_up": draw_w_up(jax.random.fold_in(key_of[4], 71), 0),
        "w_down": bell_draw(key_of[2], (FF, MODEL_WIDTH), FF ** -0.5, 0.046875, ((0, 8), (1, 4))),
        "cotangent": bell_draw(key_of[3], (TOKENS, MODEL_WIDTH), 1.0, 6.0, ((0, 2), (1, 4))),
    }


def gelu_value(pre):
    phi = 0.5 * (1.0 + jax.scipy.special.erf(pre * 0.7071067811865476))
    return pre * phi

def gelu_slope(pre):
    phi = 0.5 * (1.0 + jax.scipy.special.erf(pre * 0.7071067811865476))
    return phi + pre * jnp.exp(-0.5 * pre * pre) * 0.3989422804014327

def rounded_term(value):
    low = lax.optimization_barrier(value.astype(jnp.bfloat16))
    return low.astype(jnp.float32)

def reference(tokens, w_up, w_down, cotangent):
    block = MODEL_WIDTH // N_TCOL
    input_float = tokens.astype(jnp.float32)
    token_mean = lax.optimization_barrier(jnp.sum(input_float, axis=1)) / MODEL_WIDTH
    var = lax.optimization_barrier(jnp.sum(input_float * input_float, axis=1)) / MODEL_WIDTH - token_mean * token_mean
    inverse_stddev = lax.rsqrt(var + 1e-05)
    centered_scaled = (input_float - token_mean[:, None]) * inverse_stddev[:, None]
    normalized_rows = centered_scaled.astype(jnp.bfloat16)

    def pre_step(index, total):
        start = (index * block).astype(jnp.int32)
        left = lax.dynamic_slice_in_dim(normalized_rows, start, block, 1)
        right = lax.dynamic_slice_in_dim(w_up, start, block, 0)
        return total + rounded_term(jnp.dot(left, right, preferred_element_type=jnp.float32))
    pre = lax.fori_loop(0, N_TCOL, pre_step, jnp.zeros((TOKENS, FF), jnp.float32))
    hidden = gelu_value(pre).astype(jnp.bfloat16)
    branch = jnp.dot(hidden, w_down, preferred_element_type=jnp.float32)
    mixed = (input_float + branch).astype(jnp.bfloat16)

    def down_step(index, total):
        start = (index * TOK_GRP).astype(jnp.int32)
        left = lax.dynamic_slice_in_dim(hidden, start, TOK_GRP, 0)
        right = lax.dynamic_slice_in_dim(cotangent, start, TOK_GRP, 0)
        part = lax.dot_general(left, right, (((0,), (0,)), ((), ())), preferred_element_type=jnp.float32)
        return total + rounded_term(part)
    grad_down = lax.fori_loop(0, N_FSDP, down_step, jnp.zeros((FF, MODEL_WIDTH), jnp.float32))

    def dh_step(index, total):
        start = (index * block).astype(jnp.int32)
        left = lax.dynamic_slice_in_dim(cotangent, start, block, 1)
        right = lax.dynamic_slice_in_dim(w_down, start, block, 1)
        part = lax.dot_general(left, right, (((1,), (1,)), ((), ())), preferred_element_type=jnp.float32)
        return total + rounded_term(part)
    dhid = lax.fori_loop(0, N_TCOL, dh_step, jnp.zeros((TOKENS, FF), jnp.float32))
    dpre = (dhid * gelu_slope(pre)).astype(jnp.bfloat16)

    def up_step(index, total):
        start = (index * TOK_GRP).astype(jnp.int32)
        left = lax.dynamic_slice_in_dim(normalized_rows, start, TOK_GRP, 0)
        right = lax.dynamic_slice_in_dim(dpre, start, TOK_GRP, 0)
        part = lax.dot_general(left, right, (((0,), (0,)), ((), ())), preferred_element_type=jnp.float32)
        return total + rounded_term(part)
    grad_up = lax.fori_loop(0, N_FSDP, up_step, jnp.zeros((MODEL_WIDTH, FF), jnp.float32))
    normed_gradient = lax.dot_general(dpre, w_up, (((1,), (1,)), ((), ())), preferred_element_type=jnp.float32)
    first_moment = lax.optimization_barrier(jnp.sum(normed_gradient, axis=1)) / MODEL_WIDTH
    second_moment = lax.optimization_barrier(jnp.sum(normed_gradient * centered_scaled, axis=1)) / MODEL_WIDTH
    input_gradient = cotangent.astype(jnp.float32) + inverse_stddev[:, None] * (normed_gradient - first_moment[:, None] - centered_scaled * second_moment[:, None])
    return (mixed, input_gradient.astype(jnp.bfloat16), grad_up.astype(jnp.bfloat16), grad_down.astype(jnp.bfloat16))
```

```python
import jax
import jax.numpy as jnp
from jax import lax
from jax.sharding import PartitionSpec as P


def gelu_value(pre):
    phi = 0.5 * (1.0 + jax.scipy.special.erf(pre * 0.7071067811865476))
    return pre * phi


def gelu_slope(pre):
    phi = 0.5 * (1.0 + jax.scipy.special.erf(pre * 0.7071067811865476))
    return phi + pre * jnp.exp(-0.5 * pre * pre) * 0.3989422804014327


def contract(left, right, left_dim, right_dim):
    return lax.dot_general(
        left, right, (((left_dim,), (right_dim,)), ((), ())), preferred_element_type=jnp.float32
    )


def local(tokens, w_up, w_down, cotangent):
    width = tokens.shape[1] * lax.axis_size("tcol")
    input_float = tokens.astype(jnp.float32)
    cot_all = lax.all_gather(cotangent, "fsdp", axis=0, tiled=True)
    sum_one, sum_two = lax.psum(
        (jnp.sum(input_float, axis=1), jnp.sum(input_float * input_float, axis=1)), "tcol"
    )
    token_mean = sum_one / width
    var = sum_two / width - token_mean * token_mean
    inverse_stddev = lax.rsqrt(var + 1e-05)
    centered_scaled = (input_float - token_mean[:, None]) * inverse_stddev[:, None]
    normalized_rows = centered_scaled.astype(jnp.bfloat16)
    normed_all = lax.all_gather(normalized_rows, "fsdp", axis=0, tiled=True)
    dhid_part = contract(cot_all, w_down, 1, 1).astype(jnp.bfloat16)
    dhid = lax.psum_scatter(dhid_part, "tcol", scatter_dimension=0, tiled=True).astype(jnp.float32)
    pre_part = contract(normed_all, w_up, 1, 0).astype(jnp.bfloat16)
    pre = lax.psum_scatter(pre_part, "tcol", scatter_dimension=0, tiled=True).astype(jnp.float32)
    hidden = lax.all_gather(gelu_value(pre).astype(jnp.bfloat16), "tcol", axis=0, tiled=True)
    dpre = lax.all_gather(
        (dhid * gelu_slope(pre)).astype(jnp.bfloat16), "tcol", axis=0, tiled=True
    )
    branch_part = contract(hidden, w_down, 1, 0).astype(jnp.bfloat16)
    branch = lax.psum_scatter(branch_part, "fsdp", scatter_dimension=0, tiled=True)
    branch = lax.psum(branch, "trow").astype(jnp.float32)
    mixed = (input_float + branch).astype(jnp.bfloat16)
    grad_down = contract(hidden, cot_all, 0, 0).astype(jnp.bfloat16)
    dnorm_part = contract(dpre, w_up, 1, 1).astype(jnp.bfloat16)
    dnorm = lax.psum_scatter(dnorm_part, "fsdp", scatter_dimension=0, tiled=True)
    normed_gradient = lax.psum(dnorm, "trow").astype(jnp.float32)
    grad_up = contract(normed_all, dpre, 0, 0).astype(jnp.bfloat16)
    mean_first, mean_second = lax.psum(
        (jnp.sum(normed_gradient, axis=1), jnp.sum(normed_gradient * centered_scaled, axis=1)),
        "tcol",
    )
    first_moment = mean_first / width
    second_moment = mean_second / width
    input_gradient = cotangent.astype(jnp.float32) + inverse_stddev[:, None] * (
        normed_gradient - first_moment[:, None] - centered_scaled * second_moment[:, None]
    )
    return (mixed, input_gradient.astype(jnp.bfloat16), grad_up, grad_down)


def solution(mesh):
    return jax.shard_map(
        local,
        mesh=mesh,
        in_specs=(
            P("fsdp", "tcol"),
            P("tcol", ("fsdp", "trow")),
            P(("fsdp", "trow"), "tcol"),
            P("fsdp", "tcol"),
        ),
        out_specs=(
            P("fsdp", "tcol"),
            P("fsdp", "tcol"),
            P("tcol", ("fsdp", "trow")),
            P(("fsdp", "trow"), "tcol"),
        ),
        check_vma=False,
    )
```

```python
import functools

import jax
import jax.numpy as jnp
from jax import lax
from jax.experimental import pallas as pl
from jax.experimental.pallas import tpu as pltpu
from jax.sharding import PartitionSpec as P


def gelu_value(pre):
    phi = 0.5 * (1.0 + lax.erf(pre * 0.7071067811865476))
    return pre * phi


def gelu_slope(pre):
    phi = 0.5 * (1.0 + lax.erf(pre * 0.7071067811865476))
    return phi + pre * jnp.exp(-0.5 * pre * pre) * 0.3989422804014327


def contract(left, right, left_dim, right_dim):
    return lax.dot_general(
        left, right, (((left_dim,), (right_dim,)), ((), ())), preferred_element_type=jnp.float32
    )


def local(tokens, w_up, w_down, cotangent):
    width = tokens.shape[1] * lax.axis_size("tcol")
    input_float = tokens.astype(jnp.float32)
    cot_all = lax.all_gather(cotangent, "fsdp", axis=0, tiled=True)
    sum_one, sum_two = lax.psum(
        (jnp.sum(input_float, axis=1), jnp.sum(input_float * input_float, axis=1)), "tcol"
    )
    token_mean = sum_one / width
    var = sum_two / width - token_mean * token_mean
    inverse_stddev = lax.rsqrt(var + 1e-05)
    centered_scaled = (input_float - token_mean[:, None]) * inverse_stddev[:, None]
    normalized_rows = centered_scaled.astype(jnp.bfloat16)
    normed_all = lax.all_gather(normalized_rows, "fsdp", axis=0, tiled=True)
    dhid_part = contract(cot_all, w_down, 1, 1).astype(jnp.bfloat16)
    dhid = lax.psum_scatter(dhid_part, "tcol", scatter_dimension=0, tiled=True).astype(jnp.float32)
    pre_part = contract(normed_all, w_up, 1, 0).astype(jnp.bfloat16)
    pre = lax.psum_scatter(pre_part, "tcol", scatter_dimension=0, tiled=True).astype(jnp.float32)
    hidden = lax.all_gather(gelu_value(pre).astype(jnp.bfloat16), "tcol", axis=0, tiled=True)
    dpre = lax.all_gather(
        (dhid * gelu_slope(pre)).astype(jnp.bfloat16), "tcol", axis=0, tiled=True
    )
    branch_part = contract(hidden, w_down, 1, 0).astype(jnp.bfloat16)
    branch = lax.psum_scatter(branch_part, "fsdp", scatter_dimension=0, tiled=True)
    branch = lax.psum(branch, "trow").astype(jnp.float32)
    mixed = (input_float + branch).astype(jnp.bfloat16)
    grad_down = contract(hidden, cot_all, 0, 0).astype(jnp.bfloat16)
    dnorm_part = contract(dpre, w_up, 1, 1).astype(jnp.bfloat16)
    dnorm = lax.psum_scatter(dnorm_part, "fsdp", scatter_dimension=0, tiled=True)
    normed_gradient = lax.psum(dnorm, "trow").astype(jnp.float32)
    grad_up = contract(normed_all, dpre, 0, 0).astype(jnp.bfloat16)
    mean_first, mean_second = lax.psum(
        (jnp.sum(normed_gradient, axis=1), jnp.sum(normed_gradient * centered_scaled, axis=1)),
        "tcol",
    )
    first_moment = mean_first / width
    second_moment = mean_second / width
    input_gradient = cotangent.astype(jnp.float32) + inverse_stddev[:, None] * (
        normed_gradient - first_moment[:, None] - centered_scaled * second_moment[:, None]
    )
    return (mixed, input_gradient.astype(jnp.bfloat16), grad_up, grad_down)


MESH = pl.DeviceIdType.MESH
BF, F32 = jnp.bfloat16, jnp.float32


def block_kernel(
    F, R, P, tok, cot, wup_h, wdn_h, mix_h, ig_h, nrm_h, cota_h, hid_h, dpr_h,
    wup, wdn, nrm, cota, hid, dpr, part, rec_r, rec_l, acc, slope, ybuf, xrec, mix, ig, dn,
    mean_s, rstd_s, st1, st2,
    load_sem, out_sem, ys, yr, st_s, st_r, fr_s, fr_r, fl_s, fl_r, ag_rs, ag_ls, ag_r, xs, xr, ms, mr,
):
    T, W = tok.shape
    H = wdn.shape[0]
    TC, TR = T // P, T // R
    K = 2 * F
    f, rr, p = lax.axis_index("fsdp"), lax.axis_index("trow"), lax.axis_index("tcol")
    sends = []

    barrier = pltpu.get_barrier_semaphore()
    for g in range(F):
        for j in range(R):
            if g or j:
                pl.semaphore_signal(
                    barrier,
                    inc=1,
                    device_id={"fsdp": lax.rem(f + g, F), "trow": lax.rem(rr + j, R)},
                    device_id_type=MESH,
                )
    for j in range(1, P):
        pl.semaphore_signal(
            barrier, inc=1, device_id={"tcol": lax.rem(p + j, P)}, device_id_type=MESH
        )
    loads = [
        pltpu.make_async_copy(wup_h, wup, load_sem.at[0]),
        pltpu.make_async_copy(wdn_h, wdn, load_sem.at[1]),
    ]
    for copy in loads:
        copy.start()

    def group(g):
        return lax.rem(f + g, F)

    def rows(g):
        return pl.ds(pl.multiple_of(group(g) * T, T), T)

    def chunk(g, c):
        return pl.ds(pl.multiple_of(group(g) * T + c * TC, TC), TC)

    def remote(src, dst, s, r, to):
        return pltpu.make_async_remote_copy(
            src_ref=src, dst_ref=dst, send_sem=s, recv_sem=r, device_id=to, device_id_type=MESH
        )

    def share(buf, m, g):
        return remote(
            buf.at[rows(0), :], buf.at[rows(0), :], ys.at[m, g], yr.at[m, g], {"fsdp": group(g)}
        )

    def arrive(buf, m, g):
        src = lax.rem(f + F - g, F)
        there = pl.ds(pl.multiple_of(src * T, T), T)
        remote(
            buf.at[there, :], buf.at[there, :], ys.at[m, g], yr.at[m, g], {"fsdp": group(g)}
        ).wait_recv()

    cota[rows(0), :] = cot[...]
    x = tok[...].astype(F32)
    s1 = jnp.sum(x, axis=1, keepdims=True)
    s2 = jnp.sum(x * x, axis=1, keepdims=True)
    lane = lax.broadcasted_iota(jnp.int32, (T, 128), 1)
    st1[0] = jnp.where(lane == 0, s1, jnp.where(lane == 1, s2, 0.0)).T[:8]
    pl.semaphore_wait(barrier, F * R - 1 + P - 1)

    def stat(buf, m, j):
        return remote(
            buf.at[0], buf.at[j], st_s.at[m, j], st_r.at[m, j], {"tcol": lax.rem(p + j, P)}
        )

    for j in range(1, P):
        stat(st1, 0, j).start()
    for g in range(1, F):
        share(cota, 1, g).start()
    total = st1[0]
    for j in range(1, P):
        stat(st1, 0, j).wait_recv()
        total = total + st1[j]
    width = W * P
    total = total.T
    mean = total[:, 0:1] / width
    var = total[:, 1:2] / width - mean * mean
    rstd = lax.rsqrt(var + 1e-05)
    mean_s[...] = jnp.broadcast_to(mean, mean_s.shape)
    rstd_s[...] = jnp.broadcast_to(rstd, rstd_s.shape)
    nrm[rows(0), :] = ((tok[...].astype(F32) - mean) * rstd).astype(BF)
    for g in range(1, F):
        share(nrm, 0, g).start()

    BN = min(H, 512)

    def partial(k):
        g, m = k // 2, k % 2
        if g:
            arrive((nrm, cota)[m], m, F - g)

        def body(i, _):
            n = pl.ds(pl.multiple_of(i * BN, BN), BN)
            if m == 0:
                out = jnp.dot(nrm[rows(g), :], wup[:, n], preferred_element_type=F32)
            else:
                out = contract(cota[rows(g), :], wdn[n, :], 1, 1)
            part[k, :, n] = out.astype(BF)
            return 0

        lax.fori_loop(0, H // BN, body, 0)

    def at(c):
        return pl.ds(pl.multiple_of(c * TC, TC), TC)

    def to_right(k, c):
        return remote(
            part.at[k, at(c), :], rec_r.at[k, c], fr_s.at[k, c], fr_r.at[k, c],
            {"tcol": lax.rem(p + 1, P)},
        )

    def to_left(k, c):
        return remote(
            part.at[k, at(c), :], rec_l.at[k, c], fl_s.at[k, c], fl_r.at[k, c],
            {"tcol": lax.rem(p + P - 1, P)},
        )

    def add(k, c, rec):
        part[k, at(c), :] = (
            part[k, at(c), :].astype(F32) + rec[k, c].astype(F32)
        ).astype(BF)

    def flow(k, t):
        @pl.when(p <= t)
        def _():
            c = P - 1 - t + p

            @pl.when(p > 0)
            def _():
                to_right(k, c).wait_recv()
                add(k, c, rec_r)

            to_right(k, c).start()

        @pl.when(p >= P - 1 - t)
        def _():
            c = t - P + 1 + p

            @pl.when(p < P - 1)
            def _():
                to_left(k, c).wait_recv()
                add(k, c, rec_l)

            to_left(k, c).start()

    def flow_end(k, t):
        @pl.when(p <= t)
        def _():
            to_right(k, P - 1 - t + p).wait_send()

        @pl.when(p >= P - 1 - t)
        def _():
            to_left(k, t - P + 1 + p).wait_send()

    def final(k):
        g, m = k // 2, k % 2
        acc[...] = part[k, at(p), :].astype(F32)

        @pl.when(p > 0)
        def _():
            to_right(k, p).wait_recv()
            acc[...] += rec_r[k, p].astype(F32)

        @pl.when(p < P - 1)
        def _():
            to_left(k, p).wait_recv()
            acc[...] += rec_l[k, p].astype(F32)

        def body(i, _):
            n = pl.ds(pl.multiple_of(i * BN, BN), BN)
            a = acc[:, n]
            if m == 0:
                hid[chunk(g, p), n] = gelu_value(a).astype(BF)
                slope[:, n] = gelu_slope(a)
            else:
                dpr[chunk(g, p), n] = (a * slope[:, n]).astype(BF)
            return 0

        lax.fori_loop(0, H // BN, body, 0)

    def pass_right(k, c):
        buf = (hid, dpr)[k % 2].at[chunk(k // 2, c), :]
        return remote(buf, buf, ag_rs.at[k, c], ag_r.at[k, c], {"tcol": lax.rem(p + 1, P)})

    def pass_left(k, c):
        buf = (hid, dpr)[k % 2].at[chunk(k // 2, c), :]
        return remote(buf, buf, ag_ls.at[k, c], ag_r.at[k, c], {"tcol": lax.rem(p + P - 1, P)})

    def spread(k, d):
        def right():
            if d:
                pass_right(k, p - d).wait_recv()

            @pl.when(p < P - 1)
            def _():
                pass_right(k, p - d).start()

        def left():
            if d:
                pass_left(k, p + d).wait_recv()

            @pl.when(p > 0)
            def _():
                pass_left(k, p + d).start()

        pl.when(p >= d)(right)
        pl.when(p + d <= P - 1)(left)

    def spread_end(k, d):
        @pl.when((p >= d) & (p < P - 1))
        def _():
            pass_right(k, p - d).wait_send()

        @pl.when((p + d <= P - 1) & (p > 0))
        def _():
            pass_left(k, p + d).wait_send()

    def piece(k, j):
        g, m = k // 2, k % 2
        r = lax.rem(rr + j, R)
        return remote(
            ybuf.at[k, pl.ds(pl.multiple_of(r * TR, TR), TR), :], xrec.at[m, g, j],
            xs.at[m, g, j], xr.at[m, g, j], {"fsdp": group(g), "trow": r},
        )

    BW = min(W, 256)

    def consume(k):
        g, m = k // 2, k % 2

        def body(i, _):
            n = pl.ds(pl.multiple_of(i * BW, BW), BW)
            if m == 0:
                out = jnp.dot(hid[rows(g), :], wdn[:, n], preferred_element_type=F32)
            else:
                out = contract(dpr[rows(g), :], wup[n, :], 1, 1)
            ybuf[k, :, n] = out.astype(BF)
            return 0

        lax.fori_loop(0, W // BW, body, 0)
        for j in range(R):
            if g or j:
                piece(k, j).start()

    mine = pl.ds(pl.multiple_of(rr * TR, TR), TR)

    def gather(m):
        out = ybuf[m, mine, :].astype(F32)
        for g in range(F):
            for j in range(R):
                if g or j:
                    piece(2 * g + m, j).wait_recv()
                    out = out + xrec[m, g, j].astype(F32)
        return out

    def give(m, j):
        buf = (mix, ig)[m].at[mine, :]
        return remote(buf, buf, ms.at[m, j], mr.at[m, j], {"trow": lax.rem(rr + j, R)})

    def taken(m, j):
        r = lax.rem(rr + R - j, R)
        buf = (mix, ig)[m].at[pl.ds(pl.multiple_of(r * TR, TR), TR), :]
        remote(buf, buf, ms.at[m, j], mr.at[m, j], {"trow": r}).wait_recv()

    loads[0].wait()
    partial(0)
    flow(0, 0)
    loads[1].wait()
    partial(1)
    for t in range(1, P - 1):
        flow(0, t)
    for k in range(1, K + 1):
        if k < K:
            flow(k, 0)
        final(k - 1)
        spread(k - 1, 0)
        if k >= 2:
            spread(k - 2, P - 1)
            consume(k - 2)
        if k + 1 < K:
            partial(k + 1)
        for t in range(1, P - 1):
            if k < K:
                flow(k, t)
            spread(k - 1, t)
    outs = [
        pltpu.make_async_copy(nrm, nrm_h, out_sem.at[0]),
        pltpu.make_async_copy(cota, cota_h, out_sem.at[1]),
        pltpu.make_async_copy(hid, hid_h, out_sem.at[2]),
    ]
    for copy in outs:
        copy.start()
    mix[mine, :] = (tok[mine, :].astype(F32) + gather(0)).astype(BF)
    for j in range(1, R):
        give(0, j).start()
    spread(K - 1, P - 1)
    outs.append(pltpu.make_async_copy(dpr, dpr_h, out_sem.at[3]))
    outs[-1].start()
    consume(K - 1)
    dn[...] = gather(1)
    mean_m, rstd_m = mean_s[mine, 0:1], rstd_s[mine, 0:1]
    xhat = (tok[mine, :].astype(F32) - mean_m) * rstd_m
    s1 = jnp.sum(dn[...], axis=1, keepdims=True)
    s2 = jnp.sum(dn[...] * xhat, axis=1, keepdims=True)
    lane = lax.broadcasted_iota(jnp.int32, (TR, 128), 1)
    st2[0] = jnp.where(lane == 0, s1, jnp.where(lane == 1, s2, 0.0))
    for j in range(1, P):
        stat(st2, 1, j).start()
    total = st2[0]
    for j in range(1, P):
        stat(st2, 1, j).wait_recv()
        total = total + st2[j]
    m1, m2 = total[:, 0:1] / width, total[:, 1:2] / width
    ig[mine, :] = (
        cot[mine, :].astype(F32) + rstd_m * (dn[...] - m1 - xhat * m2)
    ).astype(BF)
    for j in range(1, R):
        give(1, j).start()
    for m in range(2):
        for j in range(1, R):
            taken(m, j)
        outs.append(pltpu.make_async_copy((mix, ig)[m], (mix_h, ig_h)[m], out_sem.at[4 + m]))
        outs[-1].start()

    for g in range(1, F):
        share(nrm, 0, g).wait_send()
        share(cota, 1, g).wait_send()
    for j in range(1, P):
        stat(st1, 0, j).wait_send()
        stat(st2, 1, j).wait_send()
    for k in range(K):
        for t in range(P - 1):
            flow_end(k, t)
        for d in range(P):
            spread_end(k, d)
        for j in range(R):
            if k // 2 or j:
                piece(k, j).wait_send()
    for m in range(2):
        for j in range(1, R):
            give(m, j).wait_send()
    for copy in outs:
        copy.wait()


def fused(F, R, P_, tokens, w_up, w_down, cotangent):
    T, W = tokens.shape
    H = w_down.shape[0]
    K = 2 * F
    TC, TR = T // P_, T // R
    S = jax.ShapeDtypeStruct
    any_spec = pl.BlockSpec(memory_space=pl.ANY)
    vmem = pl.BlockSpec(memory_space=pltpu.VMEM)
    dma = pltpu.SemaphoreType.DMA
    V = pltpu.VMEM
    mixed, input_gradient, normed, cot_all, hidden, dpre = pl.pallas_call(
        functools.partial(block_kernel, F, R, P_),
        out_shape=(
            S((T, W), BF), S((T, W), BF), S((F * T, W), BF), S((F * T, W), BF),
            S((F * T, H), BF), S((F * T, H), BF),
        ),
        in_specs=[vmem, vmem, any_spec, any_spec],
        out_specs=(any_spec,) * 6,
        scratch_shapes=[
            V(w_up.shape, BF), V(w_down.shape, BF),
            V((F * T, W), BF), V((F * T, W), BF), V((F * T, H), BF), V((F * T, H), BF),
            V((K, T, H), BF), V((K, P_, TC, H), BF), V((K, P_, TC, H), BF),
            V((TC, H), F32), V((TC, H), F32),
            V((K, T, W), BF), V((2, F, R, TR, W), BF), V((T, W), BF), V((T, W), BF),
            V((TR, W), F32), V((T, 128), F32), V((T, 128), F32),
            V((P_, 8, T), F32), V((P_, TR, 128), F32),
            dma((2,)), dma((6,)), dma((2, F)), dma((2, F)), dma((2, P_)), dma((2, P_)),
            dma((K, P_)), dma((K, P_)), dma((K, P_)), dma((K, P_)),
            dma((K, P_)), dma((K, P_)), dma((K, P_)),
            dma((2, F, R)), dma((2, F, R)), dma((2, R)), dma((2, R)),
        ],
        compiler_params=pltpu.CompilerParams(
            collective_id=0, has_side_effects=True, vmem_limit_bytes=60 * 1024 * 1024
        ),
        name="ffn_block",
    )(tokens, cotangent, w_up, w_down)
    grad_down = contract(hidden, cot_all, 0, 0).astype(BF)
    grad_up = contract(normed, dpre, 0, 0).astype(BF)
    return mixed, input_gradient, grad_up, grad_down


def solution(mesh):
    F, R, P_ = mesh.shape["fsdp"], mesh.shape["trow"], mesh.shape["tcol"]
    body = functools.partial(fused, F, R, P_) if F * R <= 16 else local
    return jax.shard_map(
        body,
        mesh=mesh,
        in_specs=(
            P("fsdp", "tcol"),
            P("tcol", ("fsdp", "trow")),
            P(("fsdp", "trow"), "tcol"),
            P("fsdp", "tcol"),
        ),
        out_specs=(
            P("fsdp", "tcol"),
            P("fsdp", "tcol"),
            P("tcol", ("fsdp", "trow")),
            P(("fsdp", "trow"), "tcol"),
        ),
        check_vma=False,
    )
```

```python
import functools

import jax
import jax.numpy as jnp
from jax import lax
from jax.experimental import pallas as pl
from jax.experimental.pallas import tpu as pltpu
from jax.sharding import PartitionSpec as P


def gelu_value(pre):
    phi = 0.5 * (1.0 + lax.erf(pre * 0.7071067811865476))
    return pre * phi


def gelu_slope(pre):
    phi = 0.5 * (1.0 + lax.erf(pre * 0.7071067811865476))
    return phi + pre * jnp.exp(-0.5 * pre * pre) * 0.3989422804014327


def contract(left, right, left_dim, right_dim):
    return lax.dot_general(
        left, right, (((left_dim,), (right_dim,)), ((), ())), preferred_element_type=jnp.float32
    )


def local(tokens, w_up, w_down, cotangent):
    width = tokens.shape[1] * lax.axis_size("tcol")
    input_float = tokens.astype(jnp.float32)
    cot_all = lax.all_gather(cotangent, "fsdp", axis=0, tiled=True)
    sum_one, sum_two = lax.psum(
        (jnp.sum(input_float, axis=1), jnp.sum(input_float * input_float, axis=1)), "tcol"
    )
    token_mean = sum_one / width
    var = sum_two / width - token_mean * token_mean
    inverse_stddev = lax.rsqrt(var + 1e-05)
    centered_scaled = (input_float - token_mean[:, None]) * inverse_stddev[:, None]
    normalized_rows = centered_scaled.astype(jnp.bfloat16)
    normed_all = lax.all_gather(normalized_rows, "fsdp", axis=0, tiled=True)
    dhid_part = contract(cot_all, w_down, 1, 1).astype(jnp.bfloat16)
    dhid = lax.psum_scatter(dhid_part, "tcol", scatter_dimension=0, tiled=True).astype(jnp.float32)
    pre_part = contract(normed_all, w_up, 1, 0).astype(jnp.bfloat16)
    pre = lax.psum_scatter(pre_part, "tcol", scatter_dimension=0, tiled=True).astype(jnp.float32)
    hidden = lax.all_gather(gelu_value(pre).astype(jnp.bfloat16), "tcol", axis=0, tiled=True)
    dpre = lax.all_gather(
        (dhid * gelu_slope(pre)).astype(jnp.bfloat16), "tcol", axis=0, tiled=True
    )
    branch_part = contract(hidden, w_down, 1, 0).astype(jnp.bfloat16)
    branch = lax.psum_scatter(branch_part, "fsdp", scatter_dimension=0, tiled=True)
    branch = lax.psum(branch, "trow").astype(jnp.float32)
    mixed = (input_float + branch).astype(jnp.bfloat16)
    grad_down = contract(hidden, cot_all, 0, 0).astype(jnp.bfloat16)
    dnorm_part = contract(dpre, w_up, 1, 1).astype(jnp.bfloat16)
    dnorm = lax.psum_scatter(dnorm_part, "fsdp", scatter_dimension=0, tiled=True)
    normed_gradient = lax.psum(dnorm, "trow").astype(jnp.float32)
    grad_up = contract(normed_all, dpre, 0, 0).astype(jnp.bfloat16)
    mean_first, mean_second = lax.psum(
        (jnp.sum(normed_gradient, axis=1), jnp.sum(normed_gradient * centered_scaled, axis=1)),
        "tcol",
    )
    first_moment = mean_first / width
    second_moment = mean_second / width
    input_gradient = cotangent.astype(jnp.float32) + inverse_stddev[:, None] * (
        normed_gradient - first_moment[:, None] - centered_scaled * second_moment[:, None]
    )
    return (mixed, input_gradient.astype(jnp.bfloat16), grad_up, grad_down)


MESH = pl.DeviceIdType.MESH
BF, F32 = jnp.bfloat16, jnp.float32
HALVES, SPACING = 4, 1


def block_kernel(
    F, R, P, tok, cot, wup_h, wdn_h, mix_h, ig_h, nrm_h, cota_h, hid_h, dpr_h,
    wup, wdn, nrm, cota, hid, dpr, part, rec_r, rec_l, acc, slope, ybuf, xrec, mix, ig, dn,
    mean_s, rstd_s, st1, st2,
    load_sem, out_sem, ys, yr, st_s, st_r, fr_s, fr_r, fl_s, fl_r, ag_rs, ag_ls, ag_r, xs, xr, ms, mr,
):
    T, W = tok.shape
    H = wdn.shape[0]
    TC, TR = T // P, T // R
    TS = TC // R
    HH = H // HALVES
    rounds = [(g, m, h) for g in range(F) for m in range(2) for h in range(HALVES)]
    K = len(rounds)
    f, rr, p = lax.axis_index("fsdp"), lax.axis_index("trow"), lax.axis_index("tcol")
    sends = []

    barrier = pltpu.get_barrier_semaphore()
    for g in range(F):
        for j in range(R):
            if g or j:
                pl.semaphore_signal(
                    barrier,
                    inc=1,
                    device_id={"fsdp": lax.rem(f + g, F), "trow": lax.rem(rr + j, R)},
                    device_id_type=MESH,
                )
    for j in range(1, P):
        pl.semaphore_signal(
            barrier, inc=1, device_id={"tcol": lax.rem(p + j, P)}, device_id_type=MESH
        )
    loads = [
        pltpu.make_async_copy(wup_h, wup, load_sem.at[0]),
        pltpu.make_async_copy(wdn_h, wdn, load_sem.at[1]),
    ]
    for copy in loads:
        copy.start()

    def group(g):
        return lax.rem(f + g, F)

    def rows(g):
        return pl.ds(pl.multiple_of(group(g) * T, T), T)

    def chunk(g, c):
        return pl.ds(pl.multiple_of(group(g) * T + c * TC, TC), TC)

    def remote(src, dst, s, r, to):
        return pltpu.make_async_remote_copy(
            src_ref=src, dst_ref=dst, send_sem=s, recv_sem=r, device_id=to, device_id_type=MESH
        )

    def share(buf, m, g):
        return remote(
            buf.at[rows(0), :], buf.at[rows(0), :], ys.at[m, g], yr.at[m, g], {"fsdp": group(g)}
        )

    def arrive(buf, m, g):
        src = lax.rem(f + F - g, F)
        there = pl.ds(pl.multiple_of(src * T, T), T)
        remote(
            buf.at[there, :], buf.at[there, :], ys.at[m, g], yr.at[m, g], {"fsdp": group(g)}
        ).wait_recv()

    cota[rows(0), :] = cot[...]
    x = tok[...].astype(F32)
    s1 = jnp.sum(x, axis=1, keepdims=True)
    s2 = jnp.sum(x * x, axis=1, keepdims=True)
    lane = lax.broadcasted_iota(jnp.int32, (T, 128), 1)
    st1[0] = jnp.where(lane == 0, s1, jnp.where(lane == 1, s2, 0.0)).T[:8]
    pl.semaphore_wait(barrier, F * R - 1 + P - 1)

    def stat(buf, m, j):
        return remote(
            buf.at[0], buf.at[j], st_s.at[m, j], st_r.at[m, j], {"tcol": lax.rem(p + j, P)}
        )

    for j in range(1, P):
        stat(st1, 0, j).start()
    total = st1[0]
    for j in range(1, P):
        stat(st1, 0, j).wait_recv()
        total = total + st1[j]
    width = W * P
    total = total.T
    mean = total[:, 0:1] / width
    var = total[:, 1:2] / width - mean * mean
    rstd = lax.rsqrt(var + 1e-05)
    mean_s[...] = jnp.broadcast_to(mean, mean_s.shape)
    rstd_s[...] = jnp.broadcast_to(rstd, rstd_s.shape)
    nrm[rows(0), :] = ((tok[...].astype(F32) - mean) * rstd).astype(BF)
    for g in range(1, F):
        share(nrm, 0, g).start()
    for g in range(1, F):
        share(cota, 1, g).start()

    BN = min(HH, 512)

    def partial(k):
        g, m, h = rounds[k]
        if g and not h:
            arrive((nrm, cota)[m], m, F - g)
        if k == HALVES:
            loads[1].wait()

        def body(i, _):
            n = pl.ds(pl.multiple_of(i * BN, BN), BN)
            w = pl.ds(pl.multiple_of(h * HH + i * BN, BN), BN)
            if m == 0:
                out = jnp.dot(nrm[rows(g), :], wup[:, w], preferred_element_type=F32)
            else:
                out = contract(cota[rows(g), :], wdn[w, :], 1, 1)
            part[k, :, n] = out.astype(BF)
            return 0

        lax.fori_loop(0, HH // BN, body, 0)

    def at(c):
        return pl.ds(pl.multiple_of(c * TC, TC), TC)

    def to_right(k, c):
        return remote(
            part.at[k, at(c), :], rec_r.at[k, c], fr_s.at[k, c], fr_r.at[k, c],
            {"tcol": lax.rem(p + 1, P)},
        )

    def to_left(k, c):
        return remote(
            part.at[k, at(c), :], rec_l.at[k, c], fl_s.at[k, c], fl_r.at[k, c],
            {"tcol": lax.rem(p + P - 1, P)},
        )

    def add(k, c, rec):
        part[k, at(c), :] = (
            part[k, at(c), :].astype(F32) + rec[k, c].astype(F32)
        ).astype(BF)

    def flow(k, t):
        @pl.when(p <= t)
        def _():
            c = P - 1 - t + p

            @pl.when(p > 0)
            def _():
                to_right(k, c).wait_recv()
                add(k, c, rec_r)

            to_right(k, c).start()

        @pl.when(p >= P - 1 - t)
        def _():
            c = t - P + 1 + p

            @pl.when(p < P - 1)
            def _():
                to_left(k, c).wait_recv()
                add(k, c, rec_l)

            to_left(k, c).start()

    def flow_end(k, t):
        @pl.when(p <= t)
        def _():
            to_right(k, P - 1 - t + p).wait_send()

        @pl.when(p >= P - 1 - t)
        def _():
            to_left(k, t - P + 1 + p).wait_send()

    def final(k):
        g, m, h = rounds[k]
        acc[...] = part[k, at(p), :].astype(F32)

        @pl.when(p > 0)
        def _():
            to_right(k, p).wait_recv()
            acc[...] += rec_r[k, p].astype(F32)

        @pl.when(p < P - 1)
        def _():
            to_left(k, p).wait_recv()
            acc[...] += rec_l[k, p].astype(F32)

        def body(i, _):
            n = pl.ds(pl.multiple_of(i * BN, BN), BN)
            a = acc[:, n]
            if m == 0:
                hid[h, chunk(g, p), n] = gelu_value(a).astype(BF)
                slope[g, h, :, n] = gelu_slope(a)
            else:
                dpr[h, chunk(g, p), n] = (a * slope[g, h, :, n]).astype(BF)
            return 0

        lax.fori_loop(0, HH // BN, body, 0)

    def passed(k, c):
        g, m, h = rounds[k]
        return (hid, dpr)[m].at[h, chunk(g, c), :]

    def pass_right(k, c):
        buf = passed(k, c)
        return remote(buf, buf, ag_rs.at[k, c], ag_r.at[k, c], {"tcol": lax.rem(p + 1, P)})

    def pass_left(k, c):
        buf = passed(k, c)
        return remote(buf, buf, ag_ls.at[k, c], ag_r.at[k, c], {"tcol": lax.rem(p + P - 1, P)})

    def spread(k, d):
        def right():
            if d:
                pass_right(k, p - d).wait_recv()

            @pl.when(p < P - 1)
            def _():
                pass_right(k, p - d).start()

        def left():
            if d:
                pass_left(k, p + d).wait_recv()

            @pl.when(p > 0)
            def _():
                pass_left(k, p + d).start()

        pl.when(p >= d)(right)
        pl.when(p + d <= P - 1)(left)

    def spread_end(k, d):
        @pl.when((p >= d) & (p < P - 1))
        def _():
            pass_right(k, p - d).wait_send()

        @pl.when((p + d <= P - 1) & (p > 0))
        def _():
            pass_left(k, p + d).wait_send()

    def sub(c, r):
        return pl.ds(pl.multiple_of(c * TC + r * TS, TS), TS)

    def piece(m, g, j, c):
        r = lax.rem(rr + j, R)
        return remote(
            ybuf.at[m, g, sub(c, r), :], xrec.at[m, g, j, c],
            xs.at[m, g, j, c], xr.at[m, g, j, c], {"fsdp": group(g), "trow": r},
        )

    BW = min(W, 256)

    def project(k, c=None):
        g, m, _ = rounds[k]
        src, dst = (rows(g), pl.ds(0, T)) if c is None else (chunk(g, c), at(c))

        def body(i, _):
            n = pl.ds(pl.multiple_of(i * BW, BW), BW)
            out = 0.0
            for h in range(HALVES):
                w = slice(h * HH, (h + 1) * HH)
                if m == 0:
                    out = out + contract(hid[h, src, :], wdn[w, n], 1, 0)
                else:
                    out = out + contract(dpr[h, src, :], wup[n, w], 1, 1)
            ybuf[m, g, dst, n] = out.astype(BF)
            return 0

        lax.fori_loop(0, W // BW, body, 0)
        for j in range(R):
            if g or j:
                for cc in range(P) if c is None else (c,):
                    piece(m, g, j, cc).start()

    def consume(k):
        project(k)

    def consume_at(k, d):
        if d == 0:
            project(k, p)
        else:
            pl.when(p >= d)(lambda: project(k, p - d))
            pl.when(p + d <= P - 1)(lambda: project(k, p + d))

    def gather(m, c):
        out = ybuf[m, 0, sub(c, rr), :].astype(F32)
        for g in range(F):
            for j in range(R):
                if g or j:
                    piece(m, g, j, c).wait_recv()
                    out = out + xrec[m, g, j, c].astype(F32)
        return out

    def give(m, j, c):
        buf = (mix, ig)[m].at[sub(c, rr), :]
        return remote(buf, buf, ms.at[m, j, c], mr.at[m, j, c], {"trow": lax.rem(rr + j, R)})

    def taken(m, j, c):
        r = lax.rem(rr + R - j, R)
        buf = (mix, ig)[m].at[sub(c, r), :]
        remote(buf, buf, ms.at[m, j, c], mr.at[m, j, c], {"trow": r}).wait_recv()

    loads[0].wait()
    partial(0)
    last = 2 * (P - 1)
    ticks = (K - 1) * SPACING + last
    for tick in range(ticks):
        for k in reversed(range(K)):
            t = tick - SPACING * k
            if 0 <= t <= P - 2:
                flow(k, t)
            elif t == P - 1:
                final(k)
                spread(k, 0)
            elif P - 1 < t <= last:
                spread(k, t - P + 1)
            if P - 1 <= t and k == K - 1:
                consume_at(k, t - P + 1)
        for k in range(K):
            if tick + 1 == SPACING * k:
                partial(k)
            if tick == SPACING * k + last and rounds[k][2] == HALVES - 1:
                consume(k)
    outs = [
        pltpu.make_async_copy(nrm, nrm_h, out_sem.at[0]),
        pltpu.make_async_copy(cota, cota_h, out_sem.at[1]),
    ] + [
        pltpu.make_async_copy(hid.at[h], hid_h.at[:, pl.ds(h * HH, HH)], out_sem.at[4 + h])
        for h in range(HALVES)
    ]
    for copy in outs:
        copy.start()
    for c in range(P):
        mix[sub(c, rr), :] = (tok[sub(c, rr), :].astype(F32) + gather(0, c)).astype(BF)
        for j in range(1, R):
            give(0, j, c).start()
    spread(K - 1, P - 1)
    consume_at(K - 1, P - 1)
    for h in range(HALVES):
        outs.append(
            pltpu.make_async_copy(
                dpr.at[h], dpr_h.at[:, pl.ds(h * HH, HH)], out_sem.at[4 + HALVES + h]
            )
        )
        outs[-1].start()
    lane = lax.broadcasted_iota(jnp.int32, (TS, 128), 1)

    def xhat(c):
        return (tok[sub(c, rr), :].astype(F32) - mean_s[sub(c, rr), 0:1]) * rstd_s[sub(c, rr), 0:1]

    for c in range(P):
        d = gather(1, c)
        dn[c * TS : (c + 1) * TS, :] = d
        s1 = jnp.sum(d, axis=1, keepdims=True)
        s2 = jnp.sum(d * xhat(c), axis=1, keepdims=True)
        st2[0, c * TS : (c + 1) * TS, :] = jnp.where(
            lane == 0, s1, jnp.where(lane == 1, s2, 0.0)
        )
    for j in range(1, P):
        stat(st2, 1, j).start()
    total = st2[0]
    for j in range(1, P):
        stat(st2, 1, j).wait_recv()
        total = total + st2[j]
    for c in range(P):
        block = total[c * TS : (c + 1) * TS]
        m1, m2 = block[:, 0:1] / width, block[:, 1:2] / width
        ig[sub(c, rr), :] = (
            cot[sub(c, rr), :].astype(F32)
            + rstd_s[sub(c, rr), 0:1] * (dn[c * TS : (c + 1) * TS, :] - m1 - xhat(c) * m2)
        ).astype(BF)
        for j in range(1, R):
            give(1, j, c).start()
    for m in range(2):
        for j in range(1, R):
            for c in range(P):
                taken(m, j, c)
        outs.append(pltpu.make_async_copy((mix, ig)[m], (mix_h, ig_h)[m], out_sem.at[2 + m]))
        outs[-1].start()

    for g in range(1, F):
        share(nrm, 0, g).wait_send()
        share(cota, 1, g).wait_send()
    for j in range(1, P):
        stat(st1, 0, j).wait_send()
        stat(st2, 1, j).wait_send()
    for k in range(K):
        for t in range(P - 1):
            flow_end(k, t)
        for d in range(P):
            spread_end(k, d)
        for j in range(R):
            g, m, h = rounds[k]
            if h == 0 and (g or j):
                for c in range(P):
                    piece(m, g, j, c).wait_send()
    for m in range(2):
        for j in range(1, R):
            for c in range(P):
                give(m, j, c).wait_send()
    for copy in outs:
        copy.wait()


def fused(F, R, P_, tokens, w_up, w_down, cotangent):
    T, W = tokens.shape
    H = w_down.shape[0]
    K = 2 * F * HALVES
    HH = H // HALVES
    TC, TR = T // P_, T // R
    S = jax.ShapeDtypeStruct
    any_spec = pl.BlockSpec(memory_space=pl.ANY)
    vmem = pl.BlockSpec(memory_space=pltpu.VMEM)
    dma = pltpu.SemaphoreType.DMA
    V = pltpu.VMEM
    mixed, input_gradient, normed, cot_all, hidden, dpre = pl.pallas_call(
        functools.partial(block_kernel, F, R, P_),
        out_shape=(
            S((T, W), BF), S((T, W), BF), S((F * T, W), BF), S((F * T, W), BF),
            S((F * T, H), BF), S((F * T, H), BF),
        ),
        in_specs=[vmem, vmem, any_spec, any_spec],
        out_specs=(any_spec,) * 6,
        scratch_shapes=[
            V(w_up.shape, BF), V(w_down.shape, BF),
            V((F * T, W), BF), V((F * T, W), BF), V((HALVES, F * T, HH), BF), V((HALVES, F * T, HH), BF),
            V((K, T, HH), BF), V((K, P_, TC, HH), BF), V((K, P_, TC, HH), BF),
            V((TC, HH), F32), V((F, HALVES, TC, HH), F32),
            V((2, F, T, W), BF), V((2, F, R, P_, TC // R, W), BF), V((T, W), BF), V((T, W), BF),
            V((TR, W), F32), V((T, 128), F32), V((T, 128), F32),
            V((P_, 8, T), F32), V((P_, TR, 128), F32),
            dma((2,)), dma((4 + 2 * HALVES,)), dma((2, F)), dma((2, F)), dma((2, P_)), dma((2, P_)),
            dma((K, P_)), dma((K, P_)), dma((K, P_)), dma((K, P_)),
            dma((K, P_)), dma((K, P_)), dma((K, P_)),
            dma((2, F, R, P_)), dma((2, F, R, P_)), dma((2, R, P_)), dma((2, R, P_)),
        ],
        compiler_params=pltpu.CompilerParams(
            collective_id=0, has_side_effects=True, vmem_limit_bytes=60 * 1024 * 1024
        ),
        name="ffn_block",
    )(tokens, cotangent, w_up, w_down)
    grad_down = contract(hidden, cot_all, 0, 0).astype(BF)
    grad_up = contract(normed, dpre, 0, 0).astype(BF)
    return mixed, input_gradient, grad_up, grad_down


def solution(mesh):
    F, R, P_ = mesh.shape["fsdp"], mesh.shape["trow"], mesh.shape["tcol"]
    body = functools.partial(fused, F, R, P_) if F * R <= 16 else local
    return jax.shard_map(
        body,
        mesh=mesh,
        in_specs=(
            P("fsdp", "tcol"),
            P("tcol", ("fsdp", "trow")),
            P(("fsdp", "trow"), "tcol"),
            P("fsdp", "tcol"),
        ),
        out_specs=(
            P("fsdp", "tcol"),
            P("fsdp", "tcol"),
            P("tcol", ("fsdp", "trow")),
            P(("fsdp", "trow"), "tcol"),
        ),
        check_vma=False,
    )
```
